32 devices in a mesh: dp: 4 (over x, core), feat: 8 (over z, y).
Axes of the slice: x: 2, y: 2, z: 4, core: 2. Of those that a mesh axis runs over, the one named last changes fastest.
Arguments:
- features: bfloat16 [131072, 2048], P('dp', 'feat'), may hold values from -210 to 210
- labels: int32 [131072], P('dp'), may hold values from 0 to 63
- groups: int32 [131072], P('dp'), may hold values from 0 to 1023
- coefficients: float32 [2048, 64], P('feat'), may hold values from -0.125 to 0.125
- coef_momentum: float32 [2048, 64], P('feat'), may hold values from -6 to 6
- group_effects: float32 [1024, 64], P('feat'), may hold values from -4 to 4
- group_momentum: float32 [1024, 64], P('feat'), may hold values from -6 to 6
- log_scale: float32 [64], replicated, may hold values from -1.2 to 0.4
Outputs:
- new_coefficients: float32 [2048, 64], P('feat')
- new_coef_momentum: float32 [2048, 64], P('feat')
- new_group_effects: float32 [1024, 64], P('feat')
- new_group_momentum: float32 [1024, 64], P('feat')
- energy_change: float32 [], replicated
The draws below stay inside these ranges and needn't reach their ends.
All inputs are finite; a program needn't handle non-finite values.
Results may differ from the reference program's by a relative error of at most 0.001.
The reference program's roundings to bfloat16 on the way (of `residual`) count: a program that leaves them out, or rounds other values in their place, can miss the bound.
Values may be sent and summed in bfloat16 or wider, within the bound.
No kernel may reach another device: no remote copies, remote signals or barrier semaphores. Data moves between devices by JAX's collectives and lax.ppermute only.
A program may use at most 128 MiB of HBM per device.

```python
import math
import jax
import jax.numpy as jnp
import numpy as np
from jax import lax

F = 2048
K = 64
G = 1024
ROW_DEV = 32768
ROWS = 131072
N_FEAT = 8


def draw_features(key, part):
    first_key, second_key, third_key = jax.random.split(key, 3)
    values = jax.random.normal(first_key, (ROWS, F), jnp.float32)
    return jnp.clip(values, -6.0, 6.0).astype(jnp.bfloat16)


def plant(values, own_key, low, high):
    index_at = [jax.random.randint(jax.random.fold_in(own_key, axis), (), 0, length) for axis, length in enumerate(values.shape)]
    main_axis = values.shape.index(max(values.shape))
    neighbour = index_at[:main_axis] + [(index_at[main_axis] + 1) % values.shape[main_axis]] + index_at[main_axis + 1:]
    return values.at[tuple(index_at)].set(low).at[tuple(neighbour)].set(high)


def steps_of(own_key, dims, pieces, low, high):
    factor_of, own = 1.0, jax.random.fold_in(own_key, 6)
    for position, parts in pieces:
        steps = jnp.exp(jax.random.uniform(jax.random.fold_in(own, position), (parts,), jnp.float32, low / len(pieces), high / len(pieces)))
        factor_of = factor_of * jnp.repeat(steps, dims[position] // parts).reshape([-1 if axis == position else 1 for axis in range(len(dims))])
    return factor_of


def rank_table(count, slope):
    portions = [(1 << 20) // math.isqrt(grade ** slope) + 1 for grade in range(1, count + 1)]
    deviation = 1 + sum(portions) // (1 << 30)
    return np.cumsum(np.array([max(1, weight // deviation) for weight in portions]))


def ranked(stream_key, dims, amount, lean):
    grid = rank_table(amount, lean)
    lot = jax.random.randint(jax.random.fold_in(stream_key, 1), dims, 0, int(grid[amount - 1]))
    rank = jnp.searchsorted(jnp.asarray(grid, jnp.int32), lot, side="right")
    return jax.random.permutation(jax.random.fold_in(stream_key, 2), amount)[rank].astype(jnp.int32)


def normal_values(own_key, extent, spread, limit, cuts=(), kind=jnp.bfloat16):
    loudness = steps_of(own_key, extent, cuts, -0.22, 0.18) if cuts else 1.0
    entries = jax.random.normal(own_key, extent, jnp.float32) * spread * loudness
    return jnp.minimum(jnp.maximum(entries, -limit), limit).astype(kind)


def setup_inputs(seed: int = 0) -> dict:
    seeds = jax.random.split(jax.random.key(seed), 9)
    return {
        "features": draw_features(jax.random.fold_in(seeds[8], 71), 0),
        "labels": plant(jax.random.randint(seeds[1], (ROWS,), 0, K), jax.random.fold_in(seeds[1], 1), 0, K - 1).astype(jnp.int32),
        "groups": plant(ranked(seeds[2], (ROWS,), G, 1), jax.random.fold_in(seeds[2], 3), 0, G - 1).astype(jnp.int32),
        "coefficients": normal_values(seeds[3], (F, K), F ** -0.5, 0.125, ((0, 8),), jnp.float32),
        "coef_momentum": normal_values(seeds[4], (F, K), 1.0, 6.0, ((0, 8),), jnp.float32),
        "group_effects": normal_values(seeds[5], (G, K), 0.5, 4.0, ((0, 8),), jnp.float32),
        "group_momentum": normal_values(seeds[6], (G, K), 1.0, 6.0, ((0, 8),), jnp.float32),
        "log_scale": jnp.clip(jax.random.uniform(seeds[7], (K,), jnp.float32, -1.2, 0.4), -1.2, 0.4),
    }


def row_terms(logits, labels):
    largest = lax.optimization_barrier(jnp.max(logits, axis=1, keepdims=True))
    shifted = logits - largest
    scaled = jnp.exp(shifted)
    normalizer = lax.optimization_barrier(jnp.sum(scaled, axis=1, keepdims=True))
    probability = scaled / normalizer
    target = (labels[:, None] == jnp.arange(K, dtype=jnp.int32)[None, :]).astype(jnp.float32)
    loglik = lax.optimization_barrier(jnp.sum(target * shifted, axis=1)) - jnp.log(normalizer[:, 0])
    residual = (target - probability).astype(jnp.bfloat16).astype(jnp.float32)
    return (loglik, residual)

def evaluate(features, labels, groups, coefficients, group_effects):
    block_rows = ROW_DEV // N_FEAT
    block_count = ROWS // block_rows
    feat_block = F // N_FEAT
    group_block = G // N_FEAT
    coef_low = coefficients.astype(jnp.bfloat16).astype(jnp.float32).reshape(N_FEAT, feat_block, K)
    group_low = group_effects.astype(jnp.bfloat16).astype(jnp.float32).reshape(N_FEAT, group_block, K)
    highest = lax.Precision.HIGHEST

    def advance(totals, block_index):
        offset = (block_index * block_rows).astype(jnp.int32)
        rows_x = lax.dynamic_slice_in_dim(features, offset, block_rows, 0).astype(jnp.float32)
        rows_l = lax.dynamic_slice_in_dim(labels, offset, block_rows, 0)
        rows_g = lax.dynamic_slice_in_dim(groups, offset, block_rows, 0)
        onehot = (rows_g[:, None] == jnp.arange(G, dtype=jnp.int32)[None, :]).astype(jnp.float32)
        partial_value = jnp.einsum('nfi,fik->fnk', rows_x.reshape(block_rows, N_FEAT, feat_block), coef_low, precision=highest)
        partial_value = partial_value + jnp.einsum('nfg,fgk->fnk', onehot.reshape(block_rows, N_FEAT, group_block), group_low, precision=highest)
        logits = lax.optimization_barrier(jnp.sum(partial_value, axis=0))
        loglik, residual = row_terms(logits, rows_l)
        coef_grad = totals[0] + jnp.einsum('ni,nk->ik', rows_x, residual, precision=highest)
        group_grad = totals[1] + jnp.einsum('ng,nk->gk', onehot, residual, precision=highest)
        return ((coef_grad, group_grad), loglik)
    initial = (jnp.zeros((F, K), jnp.float32), jnp.zeros((G, K), jnp.float32))
    (coef_grad, group_grad), loglik = lax.scan(advance, initial, jnp.arange(block_count, dtype=jnp.int32))
    return (loglik, coef_grad, group_grad)

def reference(features, labels, groups, coefficients, coef_momentum, group_effects, group_momentum, log_scale):
    step_coef = 4.0 / math.sqrt(ROWS)
    step_group = 4.0 * math.sqrt(G / ROWS)
    inv_var = jnp.exp(-2.0 * log_scale)
    loglik_old, coef_grad, group_grad = evaluate(features, labels, groups, coefficients, group_effects)
    coef_half = coef_momentum + 0.5 * step_coef * (coef_grad - coefficients)
    group_half = group_momentum + 0.5 * step_group * (group_grad - group_effects * inv_var)
    coef_new = coefficients + step_coef * coef_half
    group_new = group_effects + step_group * group_half
    loglik_new, coef_grad, group_grad = evaluate(features, labels, groups, coef_new, group_new)
    coef_mom_new = coef_half + 0.5 * step_coef * (coef_grad - coef_new)
    group_mom_new = group_half + 0.5 * step_group * (group_grad - group_new * inv_var)
    energy = jnp.sum(loglik_old - loglik_new)
    energy = energy + 0.5 * jnp.sum(coef_new * coef_new - coefficients * coefficients)
    energy = energy + 0.5 * jnp.sum((group_new * group_new - group_effects * group_effects) * inv_var)
    energy = energy + 0.5 * jnp.sum(coef_mom_new * coef_mom_new - coef_momentum * coef_momentum)
    energy = energy + 0.5 * jnp.sum(group_mom_new * group_mom_new - group_momentum * group_momentum)
    return (coef_new, coef_mom_new, group_new, group_mom_new, energy)
```

```python
import math

import jax
import jax.numpy as jnp
from jax import lax
from jax.experimental import pallas as pl
from jax.experimental.pallas import tpu as pltpu
from jax.sharding import PartitionSpec as P

CHUNKS = 4
SWAPPED = (3,)


def bits_of(count):
    bits = count.bit_length() - 1
    assert count == 1 << bits
    return bits


def stage_order(chunk, bits):
    order = list(range(bits))
    if chunk in SWAPPED and bits > 1:
        order[0], order[1] = order[1], order[0]
    return tuple(order)


def relative_of(position, order):
    bits = len(order)
    total = 0
    for stage, bit in enumerate(order):
        total = total + (((position >> (bits - 1 - stage)) & 1) << bit)
    return total


def onehot_of(groups_row, first, width):
    ids = lax.broadcasted_iota(jnp.int32, (width, groups_row.shape[1]), 0) + first
    return jnp.where(ids == groups_row, 1.0, 0.0).astype(jnp.bfloat16)


def forward_body(me_ref, x_ref, groups_ref, coef_ref, group_ref, out_ref):
    width = group_ref.shape[1]
    onehot = onehot_of(groups_ref[0], me_ref[0] * width, width)
    part = lax.dot_general(
        coef_ref[...], x_ref[...], (((1,), (1,)), ((), ())), preferred_element_type=jnp.float32
    )
    part = part + jnp.dot(group_ref[...], onehot, preferred_element_type=jnp.float32)
    out_ref[0] = part


def backward_body(me_ref, x_ref, groups_ref, resid_ref, coef_out, group_out):
    width = group_out.shape[1]

    @pl.when(pl.program_id(0) == 0)
    def _():
        coef_out[...] = jnp.zeros_like(coef_out)
        group_out[...] = jnp.zeros_like(group_out)

    onehot = onehot_of(groups_ref[0], me_ref[0] * width, width)
    resid = resid_ref[0]
    coef_out[...] += jnp.dot(resid, x_ref[...], preferred_element_type=jnp.float32)
    group_out[...] += lax.dot_general(
        resid, onehot, (((1,), (1,)), ((), ())), preferred_element_type=jnp.float32
    )


def softmax_body(kept_ref, received_ref, labels_ref, resid_ref, loglik_ref):
    logits = kept_ref[...] + received_ref[...]
    shifted = logits - jnp.max(logits, axis=0, keepdims=True)
    scaled = jnp.exp(shifted)
    normalizer = jnp.sum(scaled, axis=0, keepdims=True)
    classes = lax.broadcasted_iota(jnp.int32, logits.shape, 0)
    target = jnp.where(classes == labels_ref[...], 1.0, 0.0)
    loglik_ref[...] = jnp.sum(target * shifted, axis=0, keepdims=True) - jnp.log(normalizer)
    resid_ref[...] = (target - scaled / normalizer).astype(jnp.bfloat16)


def forward_part(me, features, groups, coef_t, group_t, chunk, order, rows):
    blocks = 1 << len(order)
    classes, feat_block = coef_t.shape

    def block_at(i, me_ref):
        return chunk * blocks + (relative_of(i, order) ^ me_ref[0])

    return pl.pallas_call(
        forward_body,
        grid_spec=pltpu.PrefetchScalarGridSpec(
            num_scalar_prefetch=1,
            grid=(blocks,),
            in_specs=[
                pl.BlockSpec((rows, feat_block), lambda i, m: (block_at(i, m), 0)),
                pl.BlockSpec((1, 1, rows), lambda i, m: (block_at(i, m), 0, 0)),
                pl.BlockSpec(coef_t.shape, lambda i, m: (0, 0)),
                pl.BlockSpec(group_t.shape, lambda i, m: (0, 0)),
            ],
            out_specs=pl.BlockSpec((1, classes, rows), lambda i, m: (i, 0, 0)),
        ),
        out_shape=jax.ShapeDtypeStruct((blocks, classes, rows), jnp.float32),
        cost_estimate=pl.CostEstimate(
            flops=2 * blocks * rows * classes * 4 * (feat_block + group_t.shape[1]),
            bytes_accessed=blocks * rows * (feat_block * 2 + classes * 4),
            transcendentals=0,
        ),
        name="forward_part",
    )(me, features, groups, coef_t, group_t)


def backward_part(me, features, groups, resid, group_block, chunk, order, rows):
    blocks, classes, _ = resid.shape
    feat_block = features.shape[1]

    def block_at(i, me_ref):
        return chunk * blocks + (relative_of(i, order) ^ me_ref[0])

    return pl.pallas_call(
        backward_body,
        grid_spec=pltpu.PrefetchScalarGridSpec(
            num_scalar_prefetch=1,
            grid=(blocks,),
            in_specs=[
                pl.BlockSpec((rows, feat_block), lambda i, m: (block_at(i, m), 0)),
                pl.BlockSpec((1, 1, rows), lambda i, m: (block_at(i, m), 0, 0)),
                pl.BlockSpec((1, classes, rows), lambda i, m: (i, 0, 0)),
            ],
            out_specs=[
                pl.BlockSpec((classes, feat_block), lambda i, m: (0, 0)),
                pl.BlockSpec((classes, group_block), lambda i, m: (0, 0)),
            ],
        ),
        out_shape=[
            jax.ShapeDtypeStruct((classes, feat_block), jnp.float32),
            jax.ShapeDtypeStruct((classes, group_block), jnp.float32),
        ],
        cost_estimate=pl.CostEstimate(
            flops=2 * blocks * rows * classes * 4 * (feat_block + group_block),
            bytes_accessed=blocks * rows * (feat_block * 2 + classes * 2),
            transcendentals=0,
        ),
        name="backward_part",
    )(me, features, groups, resid)


def softmax_part(kept, received, labels_row):
    return pl.pallas_call(
        softmax_body,
        out_shape=[
            jax.ShapeDtypeStruct(kept.shape, jnp.bfloat16),
            jax.ShapeDtypeStruct(labels_row.shape, jnp.float32),
        ],
        cost_estimate=pl.CostEstimate(
            flops=kept.size * 2000, bytes_accessed=kept.size * 10, transcendentals=kept.size
        ),
        name="softmax_part",
    )(kept, received, labels_row)


def swap(value, axis, bit):
    count = lax.axis_size(axis)
    return lax.ppermute(value, axis, [(i, i ^ (1 << bit)) for i in range(count)])


def evaluate(me, features, groups, labels_mine, coef_now, group_now):
    blocks = lax.axis_size("feat")
    bits = bits_of(blocks)
    rows = groups.shape[2]
    coef_t = coef_now.astype(jnp.bfloat16).T
    group_t = group_now.astype(jnp.bfloat16).T
    orders = [stage_order(chunk, bits) for chunk in range(CHUNKS)]
    parts = [
        forward_part(me, features, groups, coef_t, group_t, chunk, orders[chunk], rows)
        for chunk in range(CHUNKS)
    ]
    received = [None] * CHUNKS
    for stage in range(bits):
        for chunk in range(CHUNKS):
            half = parts[chunk].shape[0] // 2
            arrived = swap(parts[chunk][half:], "feat", orders[chunk][stage])
            if stage == bits - 1:
                received[chunk] = arrived
                parts[chunk] = parts[chunk][:half]
            else:
                parts[chunk] = parts[chunk][:half] + arrived
    loglik = 0.0
    resids = []
    for chunk in range(CHUNKS):
        if bits:
            kept, arrived = parts[chunk][0], received[chunk][0]
        else:
            kept, arrived = parts[chunk][0], jnp.zeros_like(parts[chunk][0])
        resid, terms = softmax_part(kept, arrived, labels_mine[chunk])
        loglik = loglik + jnp.sum(terms)
        resids.append(resid[None])
    for stage in reversed(range(bits)):
        for chunk in range(CHUNKS):
            arrived = swap(resids[chunk], "feat", orders[chunk][stage])
            resids[chunk] = jnp.concatenate([resids[chunk], arrived], axis=0)
    coef_grad, group_grad = 0.0, 0.0
    for chunk in range(CHUNKS):
        coef_add, group_add = backward_part(
            me, features, groups, resids[chunk], group_now.shape[0], chunk, orders[chunk], rows
        )
        coef_grad = coef_grad + coef_add
        group_grad = group_grad + group_add
    both = jnp.concatenate([coef_grad, group_grad], axis=1)
    for bit in range(bits_of(lax.axis_size("dp"))):
        both = both + swap(both, "dp", bit)
    coef_grad = both[:, : coef_now.shape[0]].T
    group_grad = both[:, coef_now.shape[0] :].T
    return (loglik, coef_grad, group_grad)


def per_device(
    features, labels, groups, coefficients, coef_momentum, group_effects, group_momentum, log_scale
):
    blocks = lax.axis_size("feat")
    rows_total = labels.shape[0] * lax.axis_size("dp")
    group_total = group_effects.shape[0] * blocks
    step_coef = 4.0 / math.sqrt(rows_total)
    step_group = 4.0 * math.sqrt(group_total / rows_total)
    inv_var = jnp.exp(-2.0 * log_scale)
    rows = labels.shape[0] // (blocks * CHUNKS)
    index = lax.axis_index("feat")
    me = index.astype(jnp.int32).reshape(1)
    groups_blocks = groups.reshape(CHUNKS * blocks, 1, rows)
    labels_mine = lax.dynamic_index_in_dim(
        labels.reshape(CHUNKS, blocks, rows), index, axis=1, keepdims=True
    )

    def run(coef_now, group_now):
        return evaluate(me, features, groups_blocks, labels_mine, coef_now, group_now)

    weight = 1.0 / lax.axis_size("dp")
    loglik_old, coef_grad, group_grad = run(coefficients, group_effects)
    coef_half = coef_momentum + 0.5 * step_coef * (coef_grad - coefficients)
    group_half = group_momentum + 0.5 * step_group * (group_grad - group_effects * inv_var)
    coef_new = coefficients + step_coef * coef_half
    group_new = group_effects + step_group * group_half
    loglik_new, coef_grad, group_grad = run(coef_new, group_new)
    coef_mom_new = coef_half + 0.5 * step_coef * (coef_grad - coef_new)
    group_mom_new = group_half + 0.5 * step_group * (group_grad - group_new * inv_var)
    state_terms = 0.5 * jnp.sum(coef_new * coef_new - coefficients * coefficients)
    state_terms = state_terms + 0.5 * jnp.sum(
        (group_new * group_new - group_effects * group_effects) * inv_var
    )
    state_terms = state_terms + 0.5 * jnp.sum(
        coef_mom_new * coef_mom_new - coef_momentum * coef_momentum
    )
    state_terms = state_terms + 0.5 * jnp.sum(
        group_mom_new * group_mom_new - group_momentum * group_momentum
    )
    local_terms = loglik_old - loglik_new + weight * state_terms
    energy = lax.psum(local_terms.reshape(1), ("dp", "feat"))[0]
    return (coef_new, coef_mom_new, group_new, group_mom_new, energy)


def solution(mesh):
    placed = (
        P("dp", "feat"),
        P("dp"),
        P("dp"),
        P("feat", None),
        P("feat", None),
        P("feat", None),
        P("feat", None),
        P(),
    )
    return jax.shard_map(
        per_device,
        mesh=mesh,
        in_specs=placed,
        out_specs=(P("feat", None), P("feat", None), P("feat", None), P("feat", None), P()),
        check_vma=False,
    )
```

```python
import math

import jax
import jax.numpy as jnp
from jax import lax
from jax.experimental import pallas as pl
from jax.experimental.pallas import tpu as pltpu
from jax.sharding import PartitionSpec as P

CHUNKS = 4
SWAPPED = (3,)
STARTS = (0, 1, 2, 0)


def bits_of(count):
    bits = count.bit_length() - 1
    assert count == 1 << bits
    return bits


def stage_order(chunk, bits):
    order = list(range(bits))
    if chunk in SWAPPED and bits > 1:
        order[0], order[1] = order[1], order[0]
    return tuple(order)


def relative_of(position, order):
    bits = len(order)
    total = 0
    for stage, bit in enumerate(order):
        total = total + (((position >> (bits - 1 - stage)) & 1) << bit)
    return total


def onehot_of(groups_row, first, width):
    ids = lax.broadcasted_iota(jnp.int32, (width, groups_row.shape[1]), 0) + first
    return jnp.where(ids == groups_row, 1.0, 0.0).astype(jnp.bfloat16)


def forward_body(me_ref, x_ref, groups_ref, coef_ref, group_ref, out_ref):
    width = group_ref.shape[1]
    onehot = onehot_of(groups_ref[0], me_ref[0] * width, width)
    part = lax.dot_general(
        coef_ref[...], x_ref[...], (((1,), (1,)), ((), ())), preferred_element_type=jnp.float32
    )
    part = part + jnp.dot(group_ref[...], onehot, preferred_element_type=jnp.float32)
    out_ref[0] = part


def backward_body(me_ref, x_ref, groups_ref, resid_ref, coef_out, group_out):
    width = group_out.shape[1]

    @pl.when(pl.program_id(0) == 0)
    def _():
        coef_out[...] = jnp.zeros_like(coef_out)
        group_out[...] = jnp.zeros_like(group_out)

    onehot = onehot_of(groups_ref[0], me_ref[0] * width, width)
    resid = resid_ref[0]
    coef_out[...] += jnp.dot(resid, x_ref[...], preferred_element_type=jnp.float32)
    group_out[...] += lax.dot_general(
        resid, onehot, (((1,), (1,)), ((), ())), preferred_element_type=jnp.float32
    )


def softmax_body(kept_ref, received_ref, labels_ref, resid_ref, loglik_ref):
    logits = kept_ref[...] + received_ref[...]
    shifted = logits - jnp.max(logits, axis=0, keepdims=True)
    scaled = jnp.exp(shifted)
    normalizer = jnp.sum(scaled, axis=0, keepdims=True)
    classes = lax.broadcasted_iota(jnp.int32, logits.shape, 0)
    target = jnp.where(classes == labels_ref[...], 1.0, 0.0)
    loglik_ref[...] = jnp.sum(target * shifted, axis=0, keepdims=True) - jnp.log(normalizer)
    resid_ref[...] = (target - scaled / normalizer).astype(jnp.bfloat16)


def forward_part(me, features, groups, coef_t, group_t, chunk, order, rows, first, count):
    blocks = 1 << len(order)
    classes, feat_block = coef_t.shape

    def block_at(i, me_ref):
        return chunk * blocks + (relative_of(i + first, order) ^ me_ref[0])

    return pl.pallas_call(
        forward_body,
        grid_spec=pltpu.PrefetchScalarGridSpec(
            num_scalar_prefetch=1,
            grid=(count,),
            in_specs=[
                pl.BlockSpec((rows, feat_block), lambda i, m: (block_at(i, m), 0)),
                pl.BlockSpec((1, 1, rows), lambda i, m: (block_at(i, m), 0, 0)),
                pl.BlockSpec(coef_t.shape, lambda i, m: (0, 0)),
                pl.BlockSpec(group_t.shape, lambda i, m: (0, 0)),
            ],
            out_specs=pl.BlockSpec((1, classes, rows), lambda i, m: (i, 0, 0)),
        ),
        out_shape=jax.ShapeDtypeStruct((count, classes, rows), jnp.float32),
        cost_estimate=pl.CostEstimate(
            flops=2 * count * rows * classes * 4 * (feat_block + group_t.shape[1]),
            bytes_accessed=count * rows * (feat_block * 2 + classes * 4),
            transcendentals=0,
        ),
        name="forward_part",
    )(me, features, groups, coef_t, group_t)


def backward_part(me, features, groups, resid, group_block, chunk, order, rows):
    blocks, classes, _ = resid.shape
    feat_block = features.shape[1]

    def block_at(i, me_ref):
        return chunk * blocks + (relative_of(i, order) ^ me_ref[0])

    return pl.pallas_call(
        backward_body,
        grid_spec=pltpu.PrefetchScalarGridSpec(
            num_scalar_prefetch=1,
            grid=(blocks,),
            in_specs=[
                pl.BlockSpec((rows, feat_block), lambda i, m: (block_at(i, m), 0)),
                pl.BlockSpec((1, 1, rows), lambda i, m: (block_at(i, m), 0, 0)),
                pl.BlockSpec((1, classes, rows), lambda i, m: (i, 0, 0)),
            ],
            out_specs=[
                pl.BlockSpec((classes, feat_block), lambda i, m: (0, 0)),
                pl.BlockSpec((classes, group_block), lambda i, m: (0, 0)),
            ],
        ),
        out_shape=[
            jax.ShapeDtypeStruct((classes, feat_block), jnp.float32),
            jax.ShapeDtypeStruct((classes, group_block), jnp.float32),
        ],
        cost_estimate=pl.CostEstimate(
            flops=2 * blocks * rows * classes * 4 * (feat_block + group_block),
            bytes_accessed=blocks * rows * (feat_block * 2 + classes * 2),
            transcendentals=0,
        ),
        name="backward_part",
    )(me, features, groups, resid)


def softmax_part(kept, received, labels_row):
    return pl.pallas_call(
        softmax_body,
        out_shape=[
            jax.ShapeDtypeStruct(kept.shape, jnp.bfloat16),
            jax.ShapeDtypeStruct(labels_row.shape, jnp.float32),
        ],
        cost_estimate=pl.CostEstimate(
            flops=kept.size * 2000, bytes_accessed=kept.size * 10, transcendentals=kept.size
        ),
        name="softmax_part",
    )(kept, received, labels_row)


def swap(value, axis, bit):
    count = lax.axis_size(axis)
    return lax.ppermute(value, axis, [(i, i ^ (1 << bit)) for i in range(count)])


def butterfly(value, axis):
    for bit in range(bits_of(lax.axis_size(axis))):
        value = value + swap(value, axis, bit)
    return value


def evaluate(me, features, groups, labels_mine, coef_now, group_now):
    blocks = lax.axis_size("feat")
    bits = bits_of(blocks)
    rows = groups.shape[2]
    coef_t = coef_now.astype(jnp.bfloat16).T
    group_t = group_now.astype(jnp.bfloat16).T
    half = blocks // 2
    orders = [stage_order(chunk, bits) for chunk in range(CHUNKS)]
    sends, keeps, grads = {}, {}, []
    loglik = 0.0
    for chunk in sorted(range(CHUNKS), key=lambda c: STARTS[c]):
        inputs = (me, features, groups, coef_t, group_t, chunk, orders[chunk], rows)
        sends[chunk] = forward_part(*inputs, half, blocks - half)
        keeps[chunk] = forward_part(*inputs, 0, half)
    for step in range(max(STARTS) + 2 * bits):
        live = [c for c in range(CHUNKS) if 0 <= step - STARTS[c] < 2 * bits]
        held = lax.optimization_barrier(tuple(sends[c] for c in live))
        arrivals = {}
        for chunk, value in zip(live, held):
            stage = step - STARTS[chunk]
            stage = stage if stage < bits else 2 * bits - 1 - stage
            sends[chunk] = value
            arrivals[chunk] = swap(value, "feat", orders[chunk][stage])
        for chunk in live:
            stage, arrived = step - STARTS[chunk], arrivals[chunk]
            if stage < bits - 1:
                total = keeps[chunk] + arrived
                middle = total.shape[0] // 2
                sends[chunk], keeps[chunk] = total[middle:], total[:middle]
            elif stage == bits - 1:
                resid, terms = softmax_part(keeps[chunk][0], arrived[0], labels_mine[chunk])
                loglik = loglik + jnp.sum(terms)
                sends[chunk] = resid[None]
            else:
                sends[chunk] = jnp.concatenate([sends[chunk], arrived], axis=0)
            if stage == 2 * bits - 1:
                grads.append(
                    backward_part(
                        me, features, groups, sends[chunk], group_now.shape[0],
                        chunk, orders[chunk], rows,
                    )
                )
    both = jnp.concatenate([sum(g[0] for g in grads), sum(g[1] for g in grads)], axis=1)
    both = butterfly(both, "dp")
    coef_grad = both[:, : coef_now.shape[0]].T
    group_grad = both[:, coef_now.shape[0] :].T
    return (loglik, coef_grad, group_grad)


def per_device(
    features, labels, groups, coefficients, coef_momentum, group_effects, group_momentum, log_scale
):
    blocks = lax.axis_size("feat")
    rows_total = labels.shape[0] * lax.axis_size("dp")
    group_total = group_effects.shape[0] * blocks
    step_coef = 4.0 / math.sqrt(rows_total)
    step_group = 4.0 * math.sqrt(group_total / rows_total)
    inv_var = jnp.exp(-2.0 * log_scale)
    rows = labels.shape[0] // (blocks * CHUNKS)
    index = lax.axis_index("feat")
    me = index.astype(jnp.int32).reshape(1)
    groups_blocks = groups.reshape(CHUNKS * blocks, 1, rows)
    labels_mine = lax.dynamic_index_in_dim(
        labels.reshape(CHUNKS, blocks, rows), index, axis=1, keepdims=True
    )

    def run(coef_now, group_now):
        return evaluate(me, features, groups_blocks, labels_mine, coef_now, group_now)

    weight = 1.0 / lax.axis_size("dp")
    loglik_old, coef_grad, group_grad = run(coefficients, group_effects)
    coef_half = coef_momentum + 0.5 * step_coef * (coef_grad - coefficients)
    group_half = group_momentum + 0.5 * step_group * (group_grad - group_effects * inv_var)
    coef_new = coefficients + step_coef * coef_half
    group_new = group_effects + step_group * group_half
    loglik_new, coef_grad, group_grad = run(coef_new, group_new)
    coef_mom_new = coef_half + 0.5 * step_coef * (coef_grad - coef_new)
    group_mom_new = group_half + 0.5 * step_group * (group_grad - group_new * inv_var)
    state_terms = 0.5 * jnp.sum(coef_new * coef_new - coefficients * coefficients)
    state_terms = state_terms + 0.5 * jnp.sum(
        (group_new * group_new - group_effects * group_effects) * inv_var
    )
    state_terms = state_terms + 0.5 * jnp.sum(
        coef_mom_new * coef_mom_new - coef_momentum * coef_momentum
    )
    state_terms = state_terms + 0.5 * jnp.sum(
        group_mom_new * group_mom_new - group_momentum * group_momentum
    )
    local_terms = loglik_old - loglik_new + weight * state_terms
    energy = butterfly(butterfly(local_terms.reshape(1), "dp"), "feat")[0]
    return (coef_new, coef_mom_new, group_new, group_mom_new, energy)


def solution(mesh):
    placed = (
        P("dp", "feat"),
        P("dp"),
        P("dp"),
        P("feat", None),
        P("feat", None),
        P("feat", None),
        P("feat", None),
        P(),
    )
    return jax.shard_map(
        per_device,
        mesh=mesh,
        in_specs=placed,
        out_specs=(P("feat", None), P("feat", None), P("feat", None), P("feat", None), P()),
        check_vma=False,
    )
```

```python
import math

import jax
import jax.numpy as jnp
from jax import lax
from jax.experimental import pallas as pl
from jax.experimental.pallas import tpu as pltpu
from jax.sharding import PartitionSpec as P

CHUNKS = 4
SWAPPED = (3,)
STARTS = (0, 1, 2, 2)


def bits_of(count):
    bits = count.bit_length() - 1
    assert count == 1 << bits
    return bits


def stage_order(chunk, bits):
    order = list(range(bits))
    if chunk in SWAPPED and bits > 1:
        order[0], order[1] = order[1], order[0]
    return tuple(order)


def relative_of(position, order):
    bits = len(order)
    total = 0
    for stage, bit in enumerate(order):
        total = total + (((position >> (bits - 1 - stage)) & 1) << bit)
    return total


def onehot_of(groups_row, first, width):
    ids = lax.broadcasted_iota(jnp.int32, (width, groups_row.shape[1]), 0) + first
    return jnp.where(ids == groups_row, 1.0, 0.0).astype(jnp.bfloat16)


def forward_body(me_ref, x_ref, groups_ref, coef_ref, group_ref, out_ref):
    width = group_ref.shape[1]
    onehot = onehot_of(groups_ref[0], me_ref[0] * width, width)
    part = lax.dot_general(
        coef_ref[...], x_ref[...], (((1,), (1,)), ((), ())), preferred_element_type=jnp.float32
    )
    part = part + jnp.dot(group_ref[...], onehot, preferred_element_type=jnp.float32)
    out_ref[0] = part


def backward_body(me_ref, x_ref, groups_ref, resid_ref, coef_out, group_out):
    width = group_out.shape[1]

    @pl.when(pl.program_id(0) == 0)
    def _():
        coef_out[...] = jnp.zeros_like(coef_out)
        group_out[...] = jnp.zeros_like(group_out)

    onehot = onehot_of(groups_ref[0], me_ref[0] * width, width)
    resid = resid_ref[0]
    coef_out[...] += jnp.dot(resid, x_ref[...], preferred_element_type=jnp.float32)
    group_out[...] += lax.dot_general(
        resid, onehot, (((1,), (1,)), ((), ())), preferred_element_type=jnp.float32
    )


def softmax_body(kept_ref, received_ref, labels_ref, resid_ref, loglik_ref):
    logits = kept_ref[...] + received_ref[...]
    shifted = logits - jnp.max(logits, axis=0, keepdims=True)
    scaled = jnp.exp(shifted)
    normalizer = jnp.sum(scaled, axis=0, keepdims=True)
    classes = lax.broadcasted_iota(jnp.int32, logits.shape, 0)
    target = jnp.where(classes == labels_ref[...], 1.0, 0.0)
    loglik_ref[...] = jnp.sum(target * shifted, axis=0, keepdims=True) - jnp.log(normalizer)
    resid_ref[...] = (target - scaled / normalizer).astype(jnp.bfloat16)


def forward_part(me, features, groups, coef_t, group_t, chunk, order, rows, first, count):
    blocks = 1 << len(order)
    classes, feat_block = coef_t.shape

    def block_at(i, me_ref):
        return chunk * blocks + (relative_of(i + first, order) ^ me_ref[0])

    return pl.pallas_call(
        forward_body,
        grid_spec=pltpu.PrefetchScalarGridSpec(
            num_scalar_prefetch=1,
            grid=(count,),
            in_specs=[
                pl.BlockSpec((rows, feat_block), lambda i, m: (block_at(i, m), 0)),
                pl.BlockSpec((1, 1, rows), lambda i, m: (block_at(i, m), 0, 0)),
                pl.BlockSpec(coef_t.shape, lambda i, m: (0, 0)),
                pl.BlockSpec(group_t.shape, lambda i, m: (0, 0)),
            ],
            out_specs=pl.BlockSpec((1, classes, rows), lambda i, m: (i, 0, 0)),
        ),
        out_shape=jax.ShapeDtypeStruct((count, classes, rows), jnp.float32),
        cost_estimate=pl.CostEstimate(
            flops=2 * count * rows * classes * 4 * (feat_block + group_t.shape[1]),
            bytes_accessed=count * rows * (feat_block * 2 + classes * 4),
            transcendentals=0,
        ),
        name="forward_part",
    )(me, features, groups, coef_t, group_t)


def backward_part(me, features, groups, resid, group_block, chunk, order, rows):
    blocks, classes, _ = resid.shape
    feat_block = features.shape[1]

    def block_at(i, me_ref):
        return chunk * blocks + (relative_of(i, order) ^ me_ref[0])

    return pl.pallas_call(
        backward_body,
        grid_spec=pltpu.PrefetchScalarGridSpec(
            num_scalar_prefetch=1,
            grid=(blocks,),
            in_specs=[
                pl.BlockSpec((rows, feat_block), lambda i, m: (block_at(i, m), 0)),
                pl.BlockSpec((1, 1, rows), lambda i, m: (block_at(i, m), 0, 0)),
                pl.BlockSpec((1, classes, rows), lambda i, m: (i, 0, 0)),
            ],
            out_specs=[
                pl.BlockSpec((classes, feat_block), lambda i, m: (0, 0)),
                pl.BlockSpec((classes, group_block), lambda i, m: (0, 0)),
            ],
        ),
        out_shape=[
            jax.ShapeDtypeStruct((classes, feat_block), jnp.float32),
            jax.ShapeDtypeStruct((classes, group_block), jnp.float32),
        ],
        cost_estimate=pl.CostEstimate(
            flops=2 * blocks * rows * classes * 4 * (feat_block + group_block),
            bytes_accessed=blocks * rows * (feat_block * 2 + classes * 2),
            transcendentals=0,
        ),
        name="backward_part",
    )(me, features, groups, resid)


def softmax_part(kept, received, labels_row):
    return pl.pallas_call(
        softmax_body,
        out_shape=[
            jax.ShapeDtypeStruct(kept.shape, jnp.bfloat16),
            jax.ShapeDtypeStruct(labels_row.shape, jnp.float32),
        ],
        cost_estimate=pl.CostEstimate(
            flops=kept.size * 2000, bytes_accessed=kept.size * 10, transcendentals=kept.size
        ),
        name="softmax_part",
    )(kept, received, labels_row)


def swap(value, axis, bit):
    count = lax.axis_size(axis)
    return lax.ppermute(value, axis, [(i, i ^ (1 << bit)) for i in range(count)])


def butterfly(value, axis):
    for bit in range(bits_of(lax.axis_size(axis))):
        value = value + swap(value, axis, bit)
    return value


def evaluate(me, features, groups, labels_mine, coef_now, group_now):
    blocks = lax.axis_size("feat")
    bits = bits_of(blocks)
    rows = groups.shape[2]
    coef_t = coef_now.astype(jnp.bfloat16).T
    group_t = group_now.astype(jnp.bfloat16).T
    half = blocks // 2
    orders = [stage_order(chunk, bits) for chunk in range(CHUNKS)]
    sends, keeps, grads = {}, {}, []
    loglik = 0.0
    for chunk in sorted(range(CHUNKS), key=lambda c: STARTS[c]):
        inputs = (me, features, groups, coef_t, group_t, chunk, orders[chunk], rows)
        sends[chunk] = forward_part(*inputs, half, blocks - half)
        keeps[chunk] = forward_part(*inputs, 0, half)
    for step in range(max(STARTS) + 2 * bits):
        live = [c for c in range(CHUNKS) if 0 <= step - STARTS[c] < 2 * bits]
        held = lax.optimization_barrier(tuple(sends[c] for c in live))
        arrivals = {}
        for chunk, value in zip(live, held):
            stage = step - STARTS[chunk]
            stage = stage if stage < bits else 2 * bits - 1 - stage
            sends[chunk] = value
            arrivals[chunk] = swap(value, "feat", orders[chunk][stage])
        for chunk in live:
            stage, arrived = step - STARTS[chunk], arrivals[chunk]
            if stage < bits - 1:
                total = keeps[chunk] + arrived
                middle = total.shape[0] // 2
                sends[chunk], keeps[chunk] = total[middle:], total[:middle]
            elif stage == bits - 1:
                resid, terms = softmax_part(keeps[chunk][0], arrived[0], labels_mine[chunk])
                loglik = loglik + jnp.sum(terms)
                sends[chunk] = resid[None]
            else:
                sends[chunk] = jnp.concatenate([sends[chunk], arrived], axis=0)
            if stage == 2 * bits - 1:
                grads.append(
                    backward_part(
                        me, features, groups, sends[chunk], group_now.shape[0],
                        chunk, orders[chunk], rows,
                    )
                )
    both = jnp.concatenate([sum(g[0] for g in grads), sum(g[1] for g in grads)], axis=1)
    both = butterfly(both, "dp")
    coef_grad = both[:, : coef_now.shape[0]].T
    group_grad = both[:, coef_now.shape[0] :].T
    return (loglik, coef_grad, group_grad)


def per_device(
    features, labels, groups, coefficients, coef_momentum, group_effects, group_momentum, log_scale
):
    blocks = lax.axis_size("feat")
    rows_total = labels.shape[0] * lax.axis_size("dp")
    group_total = group_effects.shape[0] * blocks
    step_coef = 4.0 / math.sqrt(rows_total)
    step_group = 4.0 * math.sqrt(group_total / rows_total)
    inv_var = jnp.exp(-2.0 * log_scale)
    rows = labels.shape[0] // (blocks * CHUNKS)
    index = lax.axis_index("feat")
    me = index.astype(jnp.int32).reshape(1)
    groups_blocks = groups.reshape(CHUNKS * blocks, 1, rows)
    labels_mine = lax.dynamic_index_in_dim(
        labels.reshape(CHUNKS, blocks, rows), index, axis=1, keepdims=True
    )

    def run(coef_now, group_now):
        return evaluate(me, features, groups_blocks, labels_mine, coef_now, group_now)

    weight = 1.0 / lax.axis_size("dp")
    loglik_old, coef_grad, group_grad = run(coefficients, group_effects)
    coef_half = coef_momentum + 0.5 * step_coef * (coef_grad - coefficients)
    group_half = group_momentum + 0.5 * step_group * (group_grad - group_effects * inv_var)
    coef_new = coefficients + step_coef * coef_half
    group_new = group_effects + step_group * group_half
    loglik_new, coef_grad, group_grad = run(coef_new, group_new)
    coef_mom_new = coef_half + 0.5 * step_coef * (coef_grad - coef_new)
    group_mom_new = group_half + 0.5 * step_group * (group_grad - group_new * inv_var)
    state_terms = 0.5 * jnp.sum(coef_new * coef_new - coefficients * coefficients)
    state_terms = state_terms + 0.5 * jnp.sum(
        (group_new * group_new - group_effects * group_effects) * inv_var
    )
    state_terms = state_terms + 0.5 * jnp.sum(
        coef_mom_new * coef_mom_new - coef_momentum * coef_momentum
    )
    state_terms = state_terms + 0.5 * jnp.sum(
        group_mom_new * group_mom_new - group_momentum * group_momentum
    )
    local_terms = loglik_old - loglik_new + weight * state_terms
    energy = butterfly(butterfly(local_terms.reshape(1), "dp"), "feat")[0]
    return (coef_new, coef_mom_new, group_new, group_mom_new, energy)


def solution(mesh):
    placed = (
        P("dp", "feat"),
        P("dp"),
        P("dp"),
        P("feat", None),
        P("feat", None),
        P("feat", None),
        P("feat", None),
        P(),
    )
    return jax.shard_map(
        per_device,
        mesh=mesh,
        in_specs=placed,
        out_specs=(P("feat", None), P("feat", None), P("feat", None), P("feat", None), P()),
        check_vma=False,
    )
```
